32 devices in a mesh: dp: 4 (over y, x), expert: 8 (over z, core).
Axes of the slice: x: 2, y: 2, z: 4, core: 2. Of those that a mesh axis runs over, the one named last changes fastest.
Arguments:
- tokens: bfloat16 [57344, 768], P(('dp', 'expert')), may hold values from -6 to 6
- lengths: int32 [64], P(('dp', 'expert')), may hold values from 448 to 896, as said below
- routes: int32 [57344], P(('dp', 'expert')), may hold values from 0 to 7, as said below
- slots: int32 [57344], P(('dp', 'expert')), may hold values from 0 to 140, as said below
- ln1_gain: bfloat16 [768], P(('dp', 'expert')), may hold values from 0.5 to 1.5
- ln1_bias: bfloat16 [768], P(('dp', 'expert')), may hold values from -3 to 3
- w_qkv: bfloat16 [768, 2304], P(('dp', 'expert')), may hold values from -0.21875 to 0.21875
- w_attn_out: bfloat16 [768, 768], P(('dp', 'expert')), may hold values from -3.5 to 3.5
- ln2_gain: bfloat16 [768], P(('dp', 'expert')), may hold values from 0.5 to 1.5
- ln2_bias: bfloat16 [768], P(('dp', 'expert')), may hold values from -3 to 3
- route_proj: bfloat16 [768, 16], P(('dp', 'expert')), may hold values from -0.15625 to 0.15625
- expert_embed: float32 [8, 16], replicated, may hold values from -4 to 4
- w_in: bfloat16 [8, 768, 3072], P('expert', 'dp'), may hold values from -0.21875 to 0.21875
- w_expert_out: bfloat16 [8, 3072, 768], P('expert', 'dp'), may hold values from -1.5 to 1.5
- out_grad: bfloat16 [57344, 768], P(('dp', 'expert')), may hold values from -6 to 6
Outputs:
- output: bfloat16 [57344, 768], P(('dp', 'expert'))
- input_grad: bfloat16 [57344, 768], P(('dp', 'expert'))
- ln1_gain_grad: float32 [768], P(('dp', 'expert'))
- ln1_bias_grad: float32 [768], P(('dp', 'expert'))
- w_qkv_grad: float32 [768, 2304], P(('dp', 'expert'))
- w_attn_out_grad: float32 [768, 768], P(('dp', 'expert'))
- ln2_gain_grad: float32 [768], P(('dp', 'expert'))
- ln2_bias_grad: float32 [768], P(('dp', 'expert'))
- route_proj_grad: float32 [768, 16], P(('dp', 'expert'))
- expert_embed_grad: float32 [8, 16], replicated
- w_in_grad: float32 [8, 768, 3072], P('expert', 'dp')
- w_expert_out_grad: float32 [8, 3072, 768], P('expert', 'dp')
The draws below stay inside these ranges and needn't reach their ends.
Inputs may be any that keep to these rules, and one draw needn't show every extreme that they name: `lengths`: real tokens of a sequence slot; positions from the length on are padding. `routes`: every token, padding too, names one of the 8 experts. Within one sequence slot the tokens of one expert carry the slots 0, 1, 2, ... up to 139 once each as far as they go; every further token of that expert carries 140 and is dropped.
All inputs are finite; a program needn't handle non-finite values.
Results may differ from the reference program's by a relative error of at most 0.023.
Values may be sent and summed in bfloat16 or wider, within the bound.
A program may use at most 384 MiB of HBM per device.

```python
import math
import jax
import jax.numpy as jnp
from jax import lax

D = 768
HEADS = 12
HEAD_DIM = 64
FF = 3072
ROUTE = 16
EXP_DEV = 1
SEQ = 896
MB = 2
EXPERTS = 8
SLOTS = 64
TOKENS = 57344
CAP = 140


def plan_block(block_key, hot_expert, plain_routes):
    order_key, prior_key = jax.random.split(block_key)
    places = jnp.arange(SEQ, dtype=jnp.int32)
    half_order = jax.random.permutation(order_key, SEQ // 2)
    half_rank = jnp.zeros((SEQ,), jnp.int32).at[half_order].set(jnp.arange(SEQ // 2, dtype=jnp.int32))
    is_hot = (places < SEQ // 2) & (half_rank < CAP + 1)
    routed = jnp.where(is_hot, hot_expert, plain_routes).astype(jnp.int32)
    priority = jax.random.permutation(prior_key, SEQ).astype(jnp.int32)
    sort_key = routed * SEQ + priority
    order = jnp.argsort(sort_key, stable=True)
    place_of = jnp.zeros((SEQ,), jnp.int32).at[order].set(places)
    counts = jnp.sum((routed[:, None] == jnp.arange(EXPERTS, dtype=jnp.int32)[None, :]).astype(jnp.int32), axis=0)
    starts = jnp.cumsum(counts) - counts
    slot_of = jnp.minimum(place_of - starts[routed], CAP)
    return (routed, slot_of.astype(jnp.int32))


def route_plan(key):
    base_key = jax.random.fold_in(key, 31)
    drawn_key, hot_key, blocks_key = jax.random.split(base_key, 3)
    plain_routes = jax.random.randint(drawn_key, (SLOTS, SEQ), 0, EXPERTS, dtype=jnp.int32)
    hot_table = jax.random.randint(hot_key, (SLOTS,), 0, EXPERTS, dtype=jnp.int32)
    numbers = jnp.arange(SLOTS, dtype=jnp.int32)
    group_ids = numbers // MB // (EXPERTS // EXP_DEV) * MB + numbers % MB
    hot_expert = hot_table[group_ids]
    block_keys = jax.random.split(blocks_key, SLOTS)
    return jax.vmap(plan_block)(block_keys, hot_expert, plain_routes)


def draw_routes(key, part):
    return route_plan(key)[0].reshape(-1)


def draw_slots(key, part):
    return route_plan(key)[1].reshape(-1)


def draw_lengths(key, part):
    values = jax.random.randint(jax.random.fold_in(key, 7), (SLOTS,), SEQ // 2, SEQ + 1, dtype=jnp.int32)
    return values.at[0].set(SEQ)


def raised(drawn, rng, source, target, blocks, factor):
    owner, partner = [(jnp.arange(drawn.shape[dim]) // (drawn.shape[dim] // blocks)).reshape([-1 if axis == dim else 1 for axis in range(drawn.ndim)]) for dim in (source, target)]
    chosen = jax.random.permutation(rng, blocks)[partner]
    strong = (owner == chosen) | (owner == (partner + blocks // 2) % blocks)
    return jnp.where(strong, factor * drawn, drawn)


def steps_of(own_key, shape, shards, smallest, largest):
    gain = 1.0
    for axis_at, parts in shards:
        draws = jax.random.uniform(jax.random.fold_in(jax.random.fold_in(own_key, 6), axis_at), (parts,), jnp.float32, smallest / len(shards), largest / len(shards))
        gain = gain * jnp.repeat(jnp.exp(draws), shape[axis_at] // parts).reshape((-1,) + (1,) * (len(shape) - 1 - axis_at))
    return gain


def normal_values(key, dims, width, limit, cuts=(), kind=jnp.bfloat16):
    level = steps_of(key, dims, cuts, -0.22, 0.18) if cuts else 1.0
    array = jax.random.normal(key, dims, jnp.float32) * width * level
    return jnp.minimum(jnp.maximum(array, -limit), limit).astype(kind)


def heavy_noise(own_key, dims, width, bound, shards, heavy, kind=jnp.bfloat16):
    entries = width * jax.random.normal(own_key, dims, jnp.float32)
    if shards:
        entries = entries * steps_of(own_key, dims, shards, -0.22, 0.18)
    return jnp.clip(raised(entries, jax.random.fold_in(own_key, 3), *heavy), -bound, bound).astype(kind)


def setup_inputs(seed: int = 0) -> dict:
    seeds = jax.random.split(jax.random.key(seed), 16)
    return {
        "tokens": heavy_noise(seeds[0], (TOKENS, D), 1.0, 6.0, ((0, 32),), (0, 1, 32, 2.75)),
        "lengths": draw_lengths(jax.random.fold_in(seeds[15], 71), 0),
        "routes": draw_routes(jax.random.fold_in(seeds[15], 71), 0),
        "slots": draw_slots(jax.random.fold_in(seeds[15], 71), 0),
        "ln1_gain": jnp.clip(1.0 + 0.1 * jax.random.normal(seeds[4], (D,), jnp.float32), 0.5, 1.5).astype(jnp.bfloat16),
        "ln1_bias": normal_values(seeds[5], (D,), 0.2, 3.0, ((0, 32),)),
        "w_qkv": normal_values(seeds[6], (D, 3 * D), D ** -0.5, 0.21875, ((0, 32),)),
        "w_attn_out": normal_values(seeds[7], (D, D), (D // 256) ** -0.5, 3.5, ((0, 32),)),
        "ln2_gain": jnp.clip(1.0 + 0.1 * jax.random.normal(seeds[8], (D,), jnp.float32), 0.5, 1.5).astype(jnp.bfloat16),
        "ln2_bias": normal_values(seeds[9], (D,), 0.2, 3.0, ((0, 32),)),
        "route_proj": normal_values(seeds[10], (D, ROUTE), 0.011, 0.15625, ((0, 32),)),
        "expert_embed": normal_values(seeds[11], (EXPERTS, ROUTE), 0.25, 4.0, (), jnp.float32),
        "w_in": normal_values(seeds[12], (EXPERTS, D, FF), D ** -0.5, 0.21875, ((0, 8), (1, 4))),
        "w_expert_out": normal_values(seeds[13], (EXPERTS, FF, D), (max(1, (3 * FF) // (8 * EXPERTS * EXPERTS))) ** -0.5, 1.5, ((0, 8), (1, 4))),
        "out_grad": normal_values(seeds[14], (TOKENS, D), 1.0, 6.0, ((0, 32),)),
    }


@jax.custom_vjp
def low(v):
    return lax.optimization_barrier(v.astype(jnp.bfloat16)).astype(jnp.float32)

@jax.custom_vjp
def low_back(v):
    return v

def low_keep(v):
    return (low(v), None)

def low_pass(kept, grad):
    return (grad,)

def back_keep(v):
    return (v, None)

def back_low(kept, grad):
    return (low(grad),)
low.defvjp(low_keep, low_pass)
low_back.defvjp(back_keep, back_low)
norm_eps = 1e-05
route_scale = 3.0
neg_big = -1e+30
highest = lax.Precision.HIGHEST

def layer_norm(values, gain_vec, shift_vec):
    center = values - lax.optimization_barrier(jnp.mean(values, axis=-1, keepdims=True))
    spread = lax.optimization_barrier(jnp.mean(center * center, axis=-1, keepdims=True))
    return center * lax.rsqrt(spread + norm_eps) * gain_vec + shift_vec

def unit_rows(values):
    norm_of = jnp.sqrt(lax.optimization_barrier(jnp.sum(values * values, axis=-1, keepdims=True)))
    return values / jnp.maximum(norm_of, 1.0)

def sequence_forward(params, inputs, length, routed, slot_of):
    gain_one, shift_one, qkv_full, attn_full, gain_two, shift_two, proj_full, embed_rows, win_full, wout_full = params
    score_scale = 1.0 / math.sqrt(HEAD_DIM)
    places = jnp.arange(SEQ, dtype=jnp.int32)
    normed_one = low(layer_norm(inputs, gain_one, shift_one))
    joined_qkv = low(low_back(jnp.dot(normed_one, qkv_full, precision=highest)))
    queries = joined_qkv[:, :D].reshape(SEQ, HEADS, HEAD_DIM)
    key_rows = joined_qkv[:, D:2 * D].reshape(SEQ, HEADS, HEAD_DIM)
    value_rows = joined_qkv[:, 2 * D:].reshape(SEQ, HEADS, HEAD_DIM)
    scores = low_back(jnp.einsum('qhd,khd->hqk', queries, key_rows, precision=highest) * score_scale)
    allowed = (places[None, :] <= places[:, None]) & (places[None, :] < length)
    scores = jnp.where(allowed[None], scores, neg_big)
    softmaxed = jax.nn.softmax(scores, axis=-1)
    mixed_heads = jnp.einsum('hqk,khd->qhd', low(softmaxed), value_rows, precision=highest).reshape(SEQ, D)
    mixed_heads = low(low_back(mixed_heads))
    branch_out = low_back(jnp.dot(mixed_heads, attn_full, precision=highest))
    hidden_res = inputs + branch_out
    normed_two = low(layer_norm(hidden_res, gain_two, shift_two))
    router_rows = low_back(jnp.dot(normed_two, proj_full, precision=highest))
    logits = route_scale * jnp.dot(unit_rows(router_rows), unit_rows(embed_rows).T, precision=highest)
    chances = jax.nn.softmax(logits, axis=-1)
    picked = (routed[:, None] == jnp.arange(EXPERTS, dtype=jnp.int32)[None, :]).astype(jnp.float32)
    gate_val = lax.optimization_barrier(jnp.sum(chances * picked, axis=-1))
    live_rows = (places < length) & (slot_of < CAP)
    target = routed * CAP + slot_of
    slot_table = ((target[:, None] == jnp.arange(EXPERTS * CAP, dtype=jnp.int32)[None, :]) & live_rows[:, None]).astype(jnp.float32)
    sent_rows = low_back(jnp.dot(slot_table.T, normed_two, precision=highest).reshape(EXPERTS, CAP, D))
    pre_act = low_back(jnp.einsum('ecd,edf->ecf', sent_rows, win_full, precision=highest))
    inner_act = low(jax.nn.gelu(pre_act, approximate=False))
    returned = low(low_back(jnp.einsum('ecf,efd->ecd', inner_act, wout_full, precision=highest)))
    chosen = jnp.dot(slot_table, returned.reshape(EXPERTS * CAP, D), precision=highest)
    return hidden_res + gate_val[:, None] * chosen

def reference(tokens, lengths, routes, slots, ln1_gain, ln1_bias, w_qkv, w_attn_out, ln2_gain, ln2_bias, route_proj, expert_embed, w_in, w_expert_out, out_grad):
    params = tuple((item.astype(jnp.float32) for item in (ln1_gain, ln1_bias, w_qkv, w_attn_out, ln2_gain, ln2_bias, route_proj, expert_embed, w_in, w_expert_out)))
    inputs = tokens.astype(jnp.float32).reshape(SLOTS, SEQ, D)
    routed_all = routes.reshape(SLOTS, SEQ).astype(jnp.int32)
    slot_all = slots.reshape(SLOTS, SEQ).astype(jnp.int32)

    def whole_run(params, inputs):

        def scan_step(carry_in, scan_item):
            rows_in, length, routed, slot_of = scan_item
            return (carry_in, sequence_forward(params, rows_in, length, routed, slot_of))
        _, results = lax.scan(jax.checkpoint(scan_step), jnp.zeros((), jnp.float32), (inputs, lengths.astype(jnp.int32), routed_all, slot_all))
        return results
    results, pullback = jax.vjp(whole_run, params, inputs)
    param_grads, input_grad = pullback(out_grad.astype(jnp.float32).reshape(SLOTS, SEQ, D))
    return (results.reshape(TOKENS, D).astype(jnp.bfloat16), input_grad.reshape(TOKENS, D).astype(jnp.bfloat16), param_grads[0], param_grads[1], param_grads[2], param_grads[3], param_grads[4], param_grads[5], param_grads[6], param_grads[7], param_grads[8], param_grads[9])
```

```python
import functools
import math

import jax
import jax.numpy as jnp
from jax import lax
from jax.experimental import pallas as pl
from jax.experimental.pallas import tpu as pltpu
from jax.sharding import PartitionSpec as P

D = 768
HEADS = 12
HEAD_DIM = 64
FF = 3072
ROUTE = 16
SEQ = 896
MB = 2

norm_eps = 1e-05
route_scale = 3.0
neg_big = -1e30
highest = lax.Precision.HIGHEST
bf16 = jnp.bfloat16
f32 = jnp.float32
NT = (((1,), (1,)), ((), ()))
TN = (((0,), (0,)), ((), ()))
NN = (((1,), (0,)), ((), ()))


def dot(a,b,dims=NN):
    return lax.dot_general(a,b,dims,preferred_element_type=f32)

def row_blocks(seq, block):
    return [(lo, min(lo+block, seq)) for lo in range(0, seq, block)]

def fwd_kernel(block, len_ref, q_ref, k_ref, v_ref, o_ref, lse_ref):
    seq=q_ref.shape[0]
    length=len_ref[0]
    lane=lax.broadcasted_iota(jnp.int32,(seq,128),1)
    place=lax.broadcasted_iota(jnp.int32,(seq,128),0)
    first=lane<64
    pad_bias=jnp.where(place<length,0.0,neg_big)
    q=q_ref[...].astype(f32)*0.125
    k=k_ref[...].astype(f32)
    v=v_ref[...].astype(f32)
    sides=[]
    for h in range(2):
        own=first if h==0 else jnp.logical_not(first)
        spare=lane==(64 if h==0 else 0)
        sides.append((
            jnp.where(own,q,jnp.where(spare,1.0,0.0)).astype(bf16),
            jnp.where(own,k,jnp.where(spare,pad_bias,0.0)).astype(bf16),
            jnp.where(own,v,1.0).astype(bf16)))
    for lo,hi in row_blocks(seq,block):
        n=hi-lo
        tri=lax.broadcasted_iota(jnp.int32,(n,n),1)<=lax.broadcasted_iota(jnp.int32,(n,n),0)
        outs=[]
        for qh,kh,vh in sides:
            s=dot(qh[lo:hi],kh[:hi],NT)
            edge=jnp.where(tri,s[:,lo:],neg_big)
            s=edge if lo==0 else jnp.concatenate([s[:,:lo],edge],axis=1)
            top=jnp.max(s,axis=1,keepdims=True)
            p=jnp.exp(s-top).astype(bf16)
            acc=dot(p,vh[:hi])
            total=pltpu.roll(acc,64,1)
            outs.append((acc/total, top+jnp.log(acc)))
        f=first[lo:hi]
        o_ref[lo:hi,:]=jnp.where(f,outs[0][0],outs[1][0]).astype(bf16)
        lse_ref[lo:hi,:]=jnp.where(f,outs[1][1],outs[0][1])

def attn_fwd(length, joined, block=256):
    seq=joined.shape[0]
    pairs=HEADS//2
    return pl.pallas_call(
        functools.partial(fwd_kernel,block),
        grid=(pairs,),
        in_specs=[pl.BlockSpec(memory_space=pltpu.SMEM),
            pl.BlockSpec((seq,128),lambda i:(0,i)),
            pl.BlockSpec((seq,128),lambda i:(0,i+pairs)),
            pl.BlockSpec((seq,128),lambda i:(0,i+2*pairs))],
        out_specs=[pl.BlockSpec((seq,128),lambda i:(0,i)),pl.BlockSpec((seq,128),lambda i:(0,i))],
        out_shape=[jax.ShapeDtypeStruct((seq,D),bf16),jax.ShapeDtypeStruct((seq,D),f32)],
        name="attn_fwd",
    )(length,joined,joined,joined)

def parts_of(x):
    hi=x.astype(bf16).astype(f32)
    mid=(x-hi).astype(bf16).astype(f32)
    lo=x-hi-mid
    return hi,mid,lo

def bwd_kernel(block, len_ref, q_ref, k_ref, v_ref, do_ref, o_ref, lse_ref, dq_ref, dk_ref, dv_ref, dk_acc, dv_acc):
    seq=q_ref.shape[0]
    length=len_ref[0]
    lane=lax.broadcasted_iota(jnp.int32,(seq,128),1)
    place=lax.broadcasted_iota(jnp.int32,(seq,128),0)
    first=lane<64
    pad_bias=jnp.where(place<length,0.0,neg_big)
    q=q_ref[...].astype(f32)*0.125
    k=k_ref[...].astype(f32)
    v=v_ref[...].astype(f32)
    do=do_ref[...].astype(f32)
    prod=do*o_ref[...].astype(f32)
    lse=lse_ref[...]
    sides=[]
    for h in range(2):
        own=first if h==0 else jnp.logical_not(first)
        a0=64 if h==0 else 0
        delta=jnp.sum(jnp.where(own,prod,0.0),axis=1,keepdims=True)
        l3=parts_of(lse); d3=parts_of(delta)
        is0=lane==a0; is1=lane==a0+1; is2=lane==a0+2; is3=lane==a0+3
        ones=jnp.where(is1|is2|is3,1.0,0.0)
        qa=jnp.where(own,q,jnp.where(is0,1.0,jnp.where(is1,-l3[0],jnp.where(is2,-l3[1],jnp.where(is3,-l3[2],0.0))))).astype(bf16)
        ka=jnp.where(own,k,jnp.where(is0,pad_bias,ones)).astype(bf16)
        da=jnp.where(own,do,jnp.where(is1,-d3[0],jnp.where(is2,-d3[1],jnp.where(is3,-d3[2],0.0)))).astype(bf16)
        va=jnp.where(own,v,ones).astype(bf16)
        sides.append((qa,ka,da,va,
            jnp.where(own,q,0.0).astype(bf16),
            jnp.where(own,k,0.0).astype(bf16),
            jnp.where(own,do,0.0).astype(bf16)))
    blocks=row_blocks(seq,block)
    for lo,hi in reversed(blocks):
        n=hi-lo
        tri=lax.broadcasted_iota(jnp.int32,(n,n),0)<=lax.broadcasted_iota(jnp.int32,(n,n),1)
        dq=None; dk=None; dv=None
        for qa,ka,da,va,qo,ko,do_o in sides:
            st=dot(ka[:hi],qa[lo:hi],NT)
            edge=jnp.where(tri,st[lo:],neg_big)
            st=edge if lo==0 else jnp.concatenate([st[:lo],edge],axis=0)
            pt=jnp.exp(st)
            dst=(pt*dot(va[:hi],da[lo:hi],NT)).astype(bf16)
            pb=pt.astype(bf16)
            t_v=dot(pb,do_o[lo:hi])
            t_k=dot(dst,qo[lo:hi])
            t_q=dot(dst,ko[:hi],TN)
            dv=t_v if dv is None else dv+t_v
            dk=t_k if dk is None else dk+t_k
            dq=t_q if dq is None else dq+t_q
        dq_ref[lo:hi,:]=(dq*0.125).astype(bf16)
        if (lo,hi)==blocks[-1]:
            dk_acc[...]=dk; dv_acc[...]=dv
        else:
            dk_acc[:hi,:]+=dk; dv_acc[:hi,:]+=dv
    dk_ref[...]=dk_acc[...].astype(bf16)
    dv_ref[...]=dv_acc[...].astype(bf16)

def attn_bwd(length, joined, d_mixed, mixed, lse, block=256):
    seq=joined.shape[0]
    pairs=HEADS//2
    col=pl.BlockSpec((seq,128),lambda i:(0,i))
    return pl.pallas_call(
        functools.partial(bwd_kernel,block),
        grid=(pairs,),
        in_specs=[pl.BlockSpec(memory_space=pltpu.SMEM),
            col,
            pl.BlockSpec((seq,128),lambda i:(0,i+pairs)),
            pl.BlockSpec((seq,128),lambda i:(0,i+2*pairs)),
            col,col,col],
        out_specs=[col,col,col],
        out_shape=[jax.ShapeDtypeStruct((seq,D),bf16)]*3,
        scratch_shapes=[pltpu.VMEM((seq,128),f32),pltpu.VMEM((seq,128),f32)],
        name="attn_bwd",
    )(length,joined,joined,joined,d_mixed,mixed,lse)


def layer_norm(values, gain_vec, shift_vec):
    center = values - jnp.mean(values, axis=-1, keepdims=True)
    spread = jnp.mean(center * center, axis=-1, keepdims=True)
    return center * lax.rsqrt(spread + norm_eps) * gain_vec + shift_vec


def unit_rows(values):
    norm_of = jnp.sqrt(jnp.sum(values * values, axis=-1, keepdims=True))
    return values / jnp.maximum(norm_of, 1.0)


def unit_back(values, unit, cotangent):
    norm_of = jnp.sqrt(jnp.sum(values * values, axis=-1, keepdims=True))
    along = jnp.sum(unit * cotangent, axis=-1, keepdims=True)
    return jnp.where(norm_of > 1.0, (cotangent - unit * along) / jnp.maximum(norm_of, 1.0), cotangent)


def gelu_exact(values):
    return jax.nn.gelu(values, approximate=False)


def swap(rows):
    return lax.all_to_all(rows, "expert", split_axis=0, concat_axis=0, tiled=True)


def sum_everywhere(value, sizes):
    for axis, size in sizes:
        step = 1
        while step < size:
            value = value + lax.ppermute(value, axis, [(i, i ^ step) for i in range(size)])
            step *= 2
    return value


def expert_work(arrived, upstream, win, wout, proj, embed, own):
    rows = arrived.shape[0] * arrived.shape[1]
    x = arrived.reshape(rows, D)
    up = upstream.reshape(rows, D)
    router_rows = dot(x, proj)
    unit_r = unit_rows(router_rows)
    unit_e = unit_rows(embed)
    chances = jax.nn.softmax(route_scale * jnp.dot(unit_r, unit_e.T, precision=highest), axis=-1)
    gate = jnp.sum(chances * own, axis=-1)
    pre_act = dot(x, win)
    inner_full, gelu_back = jax.vjp(gelu_exact, pre_act)
    inner = inner_full.astype(bf16)
    returned = dot(inner, wout).astype(bf16).astype(f32)
    up_wide = up.astype(f32)
    d_returned = (gate[:, None] * up_wide).astype(bf16)
    d_pre = gelu_back(dot(d_returned, wout, NT))[0].astype(bf16)
    d_gate = jnp.sum(up_wide * returned, axis=-1)
    d_logits = (route_scale * d_gate * gate)[:, None] * (own - chances)
    d_router = unit_back(
        router_rows, unit_r, jnp.dot(d_logits, unit_e, precision=highest)
    ).astype(bf16)
    d_embed = unit_back(embed, unit_e, jnp.dot(d_logits.T, unit_r, precision=highest))
    d_sent = (dot(d_pre, win, NT) + dot(d_router, proj, NT)).astype(bf16)
    y = (gate[:, None] * returned).astype(bf16)
    grads = (dot(x, d_pre, TN), dot(inner, d_returned, TN), dot(x, d_router, TN), d_embed)
    return y.reshape(arrived.shape), d_sent.reshape(arrived.shape), grads


def per_device(
    sizes,
    tokens,
    lengths,
    routes,
    slots,
    ln1_gain,
    ln1_bias,
    w_qkv,
    w_attn_out,
    ln2_gain,
    ln2_bias,
    route_proj,
    expert_embed,
    w_in,
    w_expert_out,
    out_grad,
):
    experts = expert_embed.shape[0]
    capacity = 5 * SEQ // (4 * experts)
    slot_cols = experts * capacity
    places = jnp.arange(SEQ, dtype=jnp.int32)
    columns = jnp.arange(slot_cols, dtype=jnp.int32)
    everyone = ("dp", "expert")

    vectors = jnp.stack([ln1_gain, ln1_bias, ln2_gain, ln2_bias], axis=1)
    share = jnp.concatenate([w_qkv, w_attn_out, route_proj, vectors], axis=1)
    share = jnp.pad(share, ((0, 0), (0, 3200 - share.shape[1])))
    dense = lax.all_gather(share, everyone, axis=0, tiled=True)
    qkv = dense[:, : 3 * D]
    attn_out = dense[:, 3 * D : 4 * D]
    proj = dense[:, 4 * D : 4 * D + ROUTE]
    norms = dense[:, 4 * D + ROUTE : 4 * D + ROUTE + 4].astype(f32).T
    gain_one, shift_one, gain_two, shift_two = [norms[i] for i in range(4)]
    win = lax.all_gather(w_in, "dp", axis=1, tiled=True)[0]
    wout = lax.all_gather(w_expert_out, "dp", axis=1, tiled=True)[0]
    own = (jnp.arange(experts) == lax.axis_index("expert")).astype(f32)[None, :]

    tables = []
    ups = []
    for at in range(MB):
        span = slice(at * SEQ, (at + 1) * SEQ)
        live = (places < lengths[at]) & (slots[span] < capacity)
        target = routes[span] * capacity + slots[span]
        table = ((target[:, None] == columns[None, :]) & live[:, None]).astype(bf16)
        tables.append(table)
        rows = dot(table, out_grad[span], TN).astype(bf16)
        ups.append(swap(rows.reshape(experts, capacity, D)))

    kept = []
    for at in range(MB):
        span = slice(at * SEQ, (at + 1) * SEQ)
        inputs = tokens[span].astype(f32)
        normed_one, back_one = jax.vjp(layer_norm, inputs, gain_one, shift_one)
        low_one = normed_one.astype(bf16)
        joined = dot(low_one, qkv).astype(bf16)
        mixed, lse = attn_fwd(lengths[at : at + 1], joined)
        hidden = inputs + dot(mixed, attn_out)
        normed_two, back_two = jax.vjp(layer_norm, hidden, gain_two, shift_two)
        low_two = normed_two.astype(bf16)
        rows = dot(tables[at], low_two, TN).astype(bf16)
        arrived = swap(rows.reshape(experts, capacity, D))
        kept.append((back_one, low_one, joined, mixed, lse, hidden, back_two, arrived))

    sent_back = []
    returned = []
    expert_grads = None
    for at in range(MB):
        y, d_sent, grads = expert_work(kept[at][-1], ups[at], win, wout, proj, expert_embed, own)
        sent_back.append(swap(d_sent))
        returned.append(swap(y))
        expert_grads = grads if at == 0 else tuple(a + b for a, b in zip(expert_grads, grads))
    grad_win, grad_wout, grad_proj, grad_embed = expert_grads
    win_out = lax.psum_scatter(grad_win[None].astype(bf16), "dp", scatter_dimension=1, tiled=True)
    wout_out = lax.psum_scatter(
        grad_wout[None].astype(bf16), "dp", scatter_dimension=1, tiled=True
    )
    embed_out = sum_everywhere(grad_embed, sizes)

    dense_grads = None
    in_grads = []
    outputs = []
    for at in range(MB):
        span = slice(at * SEQ, (at + 1) * SEQ)
        back_one, low_one, joined, mixed, lse, hidden, back_two, _ = kept[at]
        d_normed_two = dot(tables[at], sent_back[at].reshape(slot_cols, D))
        d_from_two, d_gain_two, d_shift_two = back_two(d_normed_two)
        d_hidden = out_grad[span].astype(f32) + d_from_two
        d_branch = d_hidden.astype(bf16)
        d_mixed = dot(d_branch, attn_out, NT).astype(bf16)
        parts = attn_bwd(lengths[at : at + 1], joined, d_mixed, mixed, lse)
        d_joined = jnp.concatenate(parts, axis=1)
        d_from_one, d_gain_one, d_shift_one = back_one(dot(d_joined, qkv, NT))
        in_grads.append((d_hidden + d_from_one).astype(bf16))
        grads = (
            dot(low_one, d_joined, TN),
            dot(mixed, d_branch, TN),
            d_gain_one,
            d_shift_one,
            d_gain_two,
            d_shift_two,
        )
        dense_grads = grads if at == 0 else tuple(a + b for a, b in zip(dense_grads, grads))
        outputs.append(
            (hidden + dot(tables[at], returned[at].reshape(slot_cols, D))).astype(bf16)
        )
    vectors = jnp.stack(dense_grads[2:], axis=1)
    packed = jnp.concatenate(
        [dense_grads[0], dense_grads[1], grad_proj, vectors], axis=1
    ).astype(bf16)
    packed = jnp.pad(packed, ((0, 0), (0, 3200 - packed.shape[1])))
    mine = lax.psum_scatter(packed, everyone, scatter_dimension=0, tiled=True).astype(f32)
    at = 4 * D + ROUTE
    return (
        jnp.concatenate(outputs, axis=0),
        jnp.concatenate(in_grads, axis=0),
        mine[:, at],
        mine[:, at + 1],
        mine[:, : 3 * D],
        mine[:, 3 * D : 4 * D],
        mine[:, at + 2],
        mine[:, at + 3],
        mine[:, 4 * D : at],
        embed_out,
        win_out.astype(f32),
        wout_out.astype(f32),
    )


def solution(mesh):
    rows = P(("dp", "expert"), None)
    flat = P(("dp", "expert"))
    bank = P("expert", "dp", None)
    sizes = (("expert", mesh.shape["expert"]), ("dp", mesh.shape["dp"]))
    return jax.shard_map(
        functools.partial(per_device, sizes),
        mesh=mesh,
        in_specs=(
            rows, flat, flat, flat, flat, flat, rows, rows, flat, flat, rows, P(), bank, bank, rows,
        ),
        out_specs=(
            rows, rows, flat, flat, rows, rows, flat, flat, rows, P(), bank, bank,
        ),
        check_vma=False,
    )
```
